32 devices in a mesh: dp: 2 (over z, core), sp: 16 (over x, y).
Axes of the slice: x: 4, y: 4, z: 1, core: 2. Of those that a mesh axis runs over, the one named last changes fastest.
The devices are a block of a 4x4x8 slice.
Arguments:
- q: bfloat16 [64, 32, 96], P('dp'), parts along dimension 0
- k: bfloat16 [64, 4096, 32, 96], P('dp', 'sp'), parts along dimension 0
- v: bfloat16 [64, 4096, 32, 96], P('dp', 'sp'), parts along dimension 0
Outputs:
- q: bfloat16 [64, 32, 96], P('dp'), parts along dimension 0
There are 2 independent parts. The reference program is written for one: setup_inputs(seed, part) draws one part's arguments, and reference() takes and returns one part's arrays. A program takes and returns all parts, laid end to end along the dimension named above; each array names one.
All inputs are finite; a program needn't handle non-finite values.
Results may differ from the reference program's by a relative error of at most 0.012.
Values are sent between devices in bfloat16 or wider.
A program may use at most 768 MiB of HBM per device.

```python
import jax
import jax.numpy as jnp

BATCH = 32
CACHE = 4096
HEADS = 32
KV_HEADS = 32
HEAD = 96


def setup_inputs(seed: int = 0, part: int = 0) -> dict:
    kq, kk, kv = (jax.random.fold_in(k, part) for k in jax.random.split(jax.random.key(seed), 3))
    return {
        "q": (3 * jax.random.normal(kq, (BATCH, HEADS, HEAD), jnp.float32)).astype(jnp.bfloat16),
        "k": jax.random.normal(kk, (BATCH, CACHE, KV_HEADS, HEAD), jnp.float32).astype(jnp.bfloat16),
        "v": jax.random.normal(kv, (BATCH, CACHE, KV_HEADS, HEAD), jnp.float32).astype(jnp.bfloat16),
    }


def einsum(form, a, b):
    return jnp.einsum(form, a.astype(jnp.float32), b.astype(jnp.float32))


def reference(q, k, v):
    grouped = q.reshape(BATCH, KV_HEADS, -1, HEAD)
    scores = einsum("bgsd,bugd->bgsu", grouped, k) * HEAD**-0.5
    weights = jax.nn.softmax(scores, -1).astype(jnp.bfloat16)
    return einsum("bgsu,bugd->bgsd", weights, v).astype(jnp.bfloat16).reshape(BATCH, HEADS, HEAD)
```

```python
import functools
import math

import jax
import jax.numpy as jnp
from jax import lax
from jax.experimental import pallas as pl
from jax.experimental.pallas import tpu as pltpu
from jax.sharding import PartitionSpec as P

MESH = pl.DeviceIdType.MESH
LANES = 128
ROWS = 8
TURN = 16
SLOTS = 4


def kernel(n, q_hbm, k_hbm, v_hbm, out_ref, q_raw, q_wide, keys, values, parts, others, done, q_sem, k_sem, v_sem, send_sem, recv_sem, out_send, out_recv, own_sem):
    batch, heads, head = q_hbm.shape
    tokens = k_hbm.shape[1]
    own = batch // n
    unit = own * heads * head
    span = ROWS * head
    me = lax.axis_index("sp")
    side = math.isqrt(n)

    def peer(step):
        if side * side != n:
            return lax.rem(me + step, n)
        x = lax.rem(me // side + step // side, side)
        y = lax.rem(lax.rem(me, side) + lax.rem(step, side), side)
        return x * side + y

    def fetch(j, slot):
        rows = pl.ds(pl.multiple_of(peer(n - 1 - j) * unit, unit), unit)
        return (
            pltpu.make_async_copy(k_hbm.at[rows], keys.at[slot], k_sem.at[slot]),
            pltpu.make_async_copy(v_hbm.at[rows], values.at[slot], v_sem.at[slot]),
        )

    q_copy = pltpu.make_async_copy(q_hbm, q_raw, q_sem)
    q_copy.start()
    for j in range(min(SLOTS, n)):
        for copy in fetch(j, j):
            copy.start()

    barrier = pltpu.get_barrier_semaphore()

    def greet(step, _):
        pl.semaphore_signal(barrier, inc=1, device_id={"sp": peer(step)}, device_id_type=MESH)
        return 0

    lax.fori_loop(1, n, greet, 0)
    q_copy.wait()
    q_wide[:, :, :head] = q_raw[...].astype(jnp.float32)
    plain = q_wide[...].reshape(batch * heads, LANES)
    turned = plain
    for row in range(1, LANES // math.gcd(head, LANES)):
        take = lax.rem(lax.broadcasted_iota(jnp.int32, plain.shape, 0), LANES // math.gcd(head, LANES)) == row
        turned = jnp.where(take, pltpu.roll(plain, row * head % LANES, 1), turned)
    q_wide[...] = turned.reshape(batch, heads, LANES)
    pl.semaphore_wait(barrier, n - 1)

    row = lax.broadcasted_iota(jnp.int32, (ROWS, LANES), 0)
    lane = lax.broadcasted_iota(jnp.int32, (ROWS, LANES), 1)
    inside = []
    for block in range(span // LANES):
        at = lane + block * LANES - row * head
        inside.append((at >= 0) & (at < head))

    def attend(step, slot):
        first = peer(step) * own
        for s in range(own):
            for g in range(heads // ROWS):
                base = (s * heads + g * ROWS) * head
                query = q_wide[first + s, pl.ds(g * ROWS, ROWS), :]
                query = jnp.concatenate([jnp.where(i, query, 0.0) for i in inside], 1).astype(jnp.bfloat16)
                scores = jnp.dot(query, keys[slot, pl.ds(base, span), :], preferred_element_type=jnp.float32)
                scores = scores * head**-0.5
                high = jnp.max(scores, -1, keepdims=True)
                weights = jnp.exp(scores - high)
                total = jnp.sum(weights, -1, keepdims=True)
                seen = lax.dot_general(
                    weights.astype(jnp.bfloat16),
                    values[slot, pl.ds(base, span), :],
                    (((1,), (1,)), ((), ())),
                    preferred_element_type=jnp.float32,
                )
                mine = seen[:, :LANES]
                for block in range(1, span // LANES):
                    mine = jnp.where(inside[block], seen[:, block * LANES : (block + 1) * LANES], mine)
                for _ in range((LANES - head) // TURN):
                    mine = pltpu.roll(mine, 0, 1, stride=TURN, stride_axis=0)
                mine = jnp.where(lane < head, mine, jnp.where(lane == head, total, high))
                parts[step, pl.ds(s * heads + g * ROWS, ROWS), :] = mine

    def send(step):
        return pltpu.make_async_remote_copy(
            src_ref=parts.at[step],
            dst_ref=others.at[step],
            send_sem=send_sem.at[step],
            recv_sem=recv_sem.at[step],
            device_id={"sp": peer(step)},
            device_id_type=MESH,
        )

    def work(j, _):
        slot = lax.rem(j, SLOTS)
        for copy in fetch(j, slot):
            copy.wait()
        attend(n - 1 - j, slot)
        send(n - 1 - j).start()

        @pl.when(j + SLOTS < n)
        def _():
            for copy in fetch(j + SLOTS, slot):
                copy.start()

        return 0

    lax.fori_loop(0, n - 1, work, 0)
    last = (n - 1) % SLOTS
    for copy in fetch(n - 1, last):
        copy.wait()
    attend(0, last)

    for step in range(1, n):
        send(step).wait_recv()
    runs = [parts[0]] + [others[step] for step in range(1, n)]
    top = functools.reduce(jnp.maximum, [run[:, head + 1 : head + 2] for run in runs])
    sums = sum(run * jnp.exp(run[:, head + 1 : head + 2] - top) for run in runs)
    result = sums[:, :head] / sums[:, head : head + 1]
    done[...] = result.astype(jnp.bfloat16).reshape(done.shape)

    mine = pl.ds(me * own, own)
    keep = pltpu.make_async_copy(done, out_ref.at[mine], own_sem)
    keep.start()

    def give(step):
        return pltpu.make_async_remote_copy(
            src_ref=done,
            dst_ref=out_ref.at[mine],
            send_sem=out_send.at[step],
            recv_sem=out_recv.at[step],
            device_id={"sp": peer(step)},
            device_id_type=MESH,
        )

    for step in reversed(range(1, n)):
        give(step).start()
    for step in range(1, n):
        send(step).wait_send()
    for step in range(1, n):
        give(step).wait()
    keep.wait()


def solution(mesh):
    n = mesh.shape["sp"]

    def step(q, k, v):
        batch, tokens, heads, head = k.shape
        own = batch // n
        rows = own * heads
        unit = rows * head
        flat = lambda x: x.transpose(0, 2, 3, 1).reshape(batch * heads * head, tokens)
        return pl.pallas_call(
            functools.partial(kernel, n),
            out_shape=jax.ShapeDtypeStruct(q.shape, jnp.bfloat16),
            in_specs=[pl.BlockSpec(memory_space=pl.ANY)] * 3,
            out_specs=pl.BlockSpec(memory_space=pl.ANY),
            scratch_shapes=[
                pltpu.VMEM(q.shape, jnp.bfloat16),
                pltpu.VMEM((batch, heads, LANES), jnp.float32),
                pltpu.VMEM((SLOTS, unit, tokens), jnp.bfloat16),
                pltpu.VMEM((SLOTS, unit, tokens), jnp.bfloat16),
                pltpu.VMEM((n, rows, LANES), jnp.float32),
                pltpu.VMEM((n, rows, LANES), jnp.float32),
                pltpu.VMEM((own, heads, head), jnp.bfloat16),
                pltpu.SemaphoreType.DMA,
                pltpu.SemaphoreType.DMA((SLOTS,)),
                pltpu.SemaphoreType.DMA((SLOTS,)),
                pltpu.SemaphoreType.DMA((n,)),
                pltpu.SemaphoreType.DMA((n,)),
                pltpu.SemaphoreType.DMA((n,)),
                pltpu.SemaphoreType.DMA((n,)),
                pltpu.SemaphoreType.DMA,
            ],
            compiler_params=pltpu.CompilerParams(collective_id=0, has_side_effects=True, vmem_limit_bytes=60 * 2**20),
        )(q, flat(k), flat(v))

    return jax.shard_map(
        step,
        mesh=mesh,
        in_specs=(P("dp", None, None), P("dp", "sp", None, None), P("dp", "sp", None, None)),
        out_specs=P("dp", None, None),
        check_vma=False,
    )
```

```python
import functools
import math

import jax
import jax.numpy as jnp
from jax import lax
from jax.experimental import pallas as pl
from jax.experimental.pallas import tpu as pltpu
from jax.sharding import PartitionSpec as P

MESH = pl.DeviceIdType.MESH
LANES = 128
ROWS = 8
CHUNK = 8
TURN = 16
SLOTS = 4


def kernel(n, q_hbm, k_hbm, v_hbm, out_ref, q_raw, q_wide, keys, values, scores, parts, others, done, q_sem, k_sem, v_sem, send_sem, recv_sem, out_send, out_recv, own_sem):
    batch, heads, head = q_hbm.shape
    tokens = k_hbm.shape[1]
    own = batch // n
    unit = own * heads * head
    span = ROWS * head
    count = own * heads
    me = lax.axis_index("sp")
    side = math.isqrt(n)

    def peer(step):
        if side * side != n:
            return lax.rem(me + step, n)
        x = lax.rem(me // side + step // side, side)
        y = lax.rem(lax.rem(me, side) + lax.rem(step, side), side)
        return x * side + y

    def fetch(source, target, sem, j, slot):
        rows = pl.ds(pl.multiple_of(peer(n - 1 - j) * unit, unit), unit)
        return pltpu.make_async_copy(source.at[rows], target.at[slot], sem.at[slot])

    q_copy = pltpu.make_async_copy(q_hbm, q_raw, q_sem)
    q_copy.start()
    for j in range(min(SLOTS, n)):
        fetch(k_hbm, keys, k_sem, j, j).start()
        fetch(v_hbm, values, v_sem, j, j).start()

    barrier = pltpu.get_barrier_semaphore()

    def greet(step, _):
        pl.semaphore_signal(barrier, inc=1, device_id={"sp": peer(step)}, device_id_type=MESH)
        return 0

    lax.fori_loop(1, n, greet, 0)
    q_copy.wait()
    q_wide[:, :, :head] = q_raw[...].astype(jnp.float32)
    plain = q_wide[...].reshape(batch * heads, LANES)
    turned = plain
    for row in range(1, LANES // math.gcd(head, LANES)):
        take = lax.rem(lax.broadcasted_iota(jnp.int32, plain.shape, 0), LANES // math.gcd(head, LANES)) == row
        turned = jnp.where(take, pltpu.roll(plain, row * head % LANES, 1), turned)
    q_wide[...] = turned.reshape(batch, heads, LANES)
    pl.semaphore_wait(barrier, n - 1)

    row = lax.broadcasted_iota(jnp.int32, (ROWS, LANES), 0)
    lane = lax.broadcasted_iota(jnp.int32, (count, LANES), 1)
    column = lax.broadcasted_iota(jnp.int32, (head, count), 1)
    inside = []
    for block in range(span // LANES):
        at = lane[:ROWS] + block * LANES - row * head
        inside.append((at >= 0) & (at < head))

    def score(step, slot, groups):
        first = peer(step) * own
        for g in groups:
            query = q_wide[first + g * ROWS // heads, pl.ds(g * ROWS % heads, ROWS), :]
            query = jnp.concatenate([jnp.where(i, query, 0.0) for i in inside], 1).astype(jnp.bfloat16)
            scores[g * ROWS : (g + 1) * ROWS, :] = jnp.dot(
                query, keys[slot, pl.ds(g * span, span), :], preferred_element_type=jnp.float32
            ) * head**-0.5

    def attend(step, slot, after):
        drawn = scores[...]
        high = jnp.max(drawn, -1, keepdims=True)
        weights = jnp.exp(drawn - high)
        total = jnp.sum(weights, -1, keepdims=True)
        for c in range(count // CHUNK):
            after(c)
            for g in range(c * CHUNK // ROWS, (c + 1) * CHUNK // ROWS):
                at = slice(g * ROWS, (g + 1) * ROWS)
                seen = lax.dot_general(
                    weights[at].astype(jnp.bfloat16),
                    values[slot, pl.ds(g * span, span), :],
                    (((1,), (1,)), ((), ())),
                    preferred_element_type=jnp.float32,
                )
                mine = seen[:, :LANES]
                for block in range(1, span // LANES):
                    mine = jnp.where(inside[block], seen[:, block * LANES : (block + 1) * LANES], mine)
                for _ in range((LANES - head) // TURN):
                    mine = pltpu.roll(mine, 0, 1, stride=TURN, stride_axis=0)
                parts[step, at, :] = jnp.where(lane[:ROWS] < head, mine, jnp.where(lane[:ROWS] == head, total[at], high[at]))

    def send(step):
        return pltpu.make_async_remote_copy(
            src_ref=parts.at[step],
            dst_ref=others.at[step],
            send_sem=send_sem.at[step],
            recv_sem=recv_sem.at[step],
            device_id={"sp": peer(step)},
            device_id_type=MESH,
        )

    def nothing(c):
        pass

    def work(j, _):
        slot, later = lax.rem(j, SLOTS), lax.rem(j + 1, SLOTS)
        fetch(k_hbm, keys, k_sem, j + 1, later).wait()
        fetch(v_hbm, values, v_sem, j, slot).wait()
        groups = count // ROWS
        chunks = count // CHUNK

        def ahead(c):
            score(n - 2 - j, later, range(c * groups // chunks, (c + 1) * groups // chunks))

        attend(n - 1 - j, slot, ahead)
        send(n - 1 - j).start()

        @pl.when(j + 1 + SLOTS < n)
        def _():
            fetch(k_hbm, keys, k_sem, j + 1 + SLOTS, later).start()

        @pl.when(j + SLOTS < n)
        def _():
            fetch(v_hbm, values, v_sem, j + SLOTS, slot).start()

        return 0

    fetch(k_hbm, keys, k_sem, 0, 0).wait()
    score(n - 1, 0, range(count // ROWS))
    if SLOTS < n:
        fetch(k_hbm, keys, k_sem, SLOTS, 0).start()
    lax.fori_loop(0, n - 1, work, 0)
    last = (n - 1) % SLOTS
    fetch(v_hbm, values, v_sem, n - 1, last).wait()
    attend(0, last, nothing)

    for step in range(1, n):
        send(step).wait_recv()
    runs = [parts[0]] + [others[step] for step in range(1, n)]
    top = functools.reduce(jnp.maximum, [run[:, head + 1 : head + 2] for run in runs])
    sums = sum(run * jnp.exp(run[:, head + 1 : head + 2] - top) for run in runs)
    result = sums[:, :head] / sums[:, head : head + 1]
    done[...] = result.astype(jnp.bfloat16).reshape(done.shape)

    mine = pl.ds(me * own, own)
    keep = pltpu.make_async_copy(done, out_ref.at[mine], own_sem)
    keep.start()

    def give(step):
        return pltpu.make_async_remote_copy(
            src_ref=done,
            dst_ref=out_ref.at[mine],
            send_sem=out_send.at[step],
            recv_sem=out_recv.at[step],
            device_id={"sp": peer(step)},
            device_id_type=MESH,
        )

    for step in reversed(range(1, n)):
        give(step).start()
    for step in range(1, n):
        send(step).wait_send()
    for step in range(1, n):
        give(step).wait()
    keep.wait()


def solution(mesh):
    n = mesh.shape["sp"]

    def step(q, k, v):
        batch, tokens, heads, head = k.shape
        own = batch // n
        rows = own * heads
        unit = rows * head
        flat = lambda x: x.transpose(0, 2, 3, 1).reshape(batch * heads * head, tokens)
        return pl.pallas_call(
            functools.partial(kernel, n),
            out_shape=jax.ShapeDtypeStruct(q.shape, jnp.bfloat16),
            in_specs=[pl.BlockSpec(memory_space=pl.ANY)] * 3,
            out_specs=pl.BlockSpec(memory_space=pl.ANY),
            scratch_shapes=[
                pltpu.VMEM(q.shape, jnp.bfloat16),
                pltpu.VMEM((batch, heads, LANES), jnp.float32),
                pltpu.VMEM((SLOTS, unit, tokens), jnp.bfloat16),
                pltpu.VMEM((SLOTS, unit, tokens), jnp.bfloat16),
                pltpu.VMEM((rows, tokens), jnp.float32),
                pltpu.VMEM((n, rows, LANES), jnp.float32),
                pltpu.VMEM((n, rows, LANES), jnp.float32),
                pltpu.VMEM((own, heads, head), jnp.bfloat16),
                pltpu.SemaphoreType.DMA,
                pltpu.SemaphoreType.DMA((SLOTS,)),
                pltpu.SemaphoreType.DMA((SLOTS,)),
                pltpu.SemaphoreType.DMA((n,)),
                pltpu.SemaphoreType.DMA((n,)),
                pltpu.SemaphoreType.DMA((n,)),
                pltpu.SemaphoreType.DMA((n,)),
                pltpu.SemaphoreType.DMA,
            ],
            compiler_params=pltpu.CompilerParams(collective_id=0, has_side_effects=True, vmem_limit_bytes=60 * 2**20),
        )(q, flat(k), flat(v))

    return jax.shard_map(
        step,
        mesh=mesh,
        in_specs=(P("dp", None, None), P("dp", "sp", None, None), P("dp", "sp", None, None)),
        out_specs=P("dp", None, None),
        check_vma=False,
    )
```

```python
import functools
import math

import jax
import jax.numpy as jnp
from jax import lax
from jax.experimental import pallas as pl
from jax.experimental.pallas import tpu as pltpu
from jax.sharding import PartitionSpec as P

MESH = pl.DeviceIdType.MESH
LANES = 128
ROWS = 8
TURN = 16
PHASES = 2
LATE = 4
SLOTS = 4


def kernel(
    n, q_hbm, k_hbm, v_hbm, out_ref, q_raw, q_wide, keys, values, weights, seen, parts, others, done, q_sem, k_sem, v_sem, send_sem, recv_sem, out_send, out_recv, own_sem
):
    batch, heads, head = q_hbm.shape
    own = batch // n
    some = heads // PHASES
    count = own * some
    groups = some // ROWS
    span = ROWS * head
    units = PHASES * (n - 1)
    me = lax.axis_index("sp")

    def peer(step):
        if n & (n - 1) == 0:
            return me ^ step
        return lax.rem(me + step, n)

    def where(j):
        if isinstance(j, int):
            return (j // (n - 1), n - 1 - j % (n - 1)) if j < units else (j - units, 0)
        phase = sum((j >= (n - 1) * p).astype(jnp.int32) for p in range(1, PHASES)) if PHASES > 1 else 0
        theirs = j < units
        return jnp.where(theirs, phase, j - units), jnp.where(theirs, n - 1 - j + phase * (n - 1), 0)

    def fetch(source, target, sem, j):
        phase, step = where(j)
        slot = j & (SLOTS - 1)
        rows = pl.ds(phase * (some * head), some * head)
        return pltpu.make_async_copy(source.at[pl.ds(peer(step) * own, own), rows], target.at[slot], sem.at[slot])

    fetch_k = functools.partial(fetch, k_hbm, keys, k_sem)
    fetch_v = functools.partial(fetch, v_hbm, values, v_sem)

    q_copy = pltpu.make_async_copy(q_hbm, q_raw, q_sem)
    q_copy.start()
    for j in range(SLOTS):
        fetch_k(j).start()
        fetch_v(j).start()

    barrier = pltpu.get_barrier_semaphore()

    def greet(step, _):
        pl.semaphore_signal(barrier, inc=1, device_id={"sp": peer(step)}, device_id_type=MESH)
        return 0

    lax.fori_loop(1, n, greet, 0)
    q_copy.wait()
    q_wide[:, :, :head] = q_raw[...].astype(jnp.float32)
    plain = q_wide[...].reshape(batch * heads, LANES)
    turned = plain
    turns = LANES // math.gcd(head, LANES)
    for row in range(1, turns):
        take = lax.rem(lax.broadcasted_iota(jnp.int32, plain.shape, 0), turns) == row
        turned = jnp.where(take, pltpu.roll(plain, row * head % LANES, 1), turned)
    q_wide[...] = turned.reshape(batch, heads, LANES)

    row = lax.broadcasted_iota(jnp.int32, (ROWS, LANES), 0)
    lane = lax.broadcasted_iota(jnp.int32, (ROWS, LANES), 1)
    inside = []
    for block in range(span // LANES):
        at = lane + block * LANES - row * head
        inside.append((at >= 0) & (at < head))

    def weigh(j, g):
        phase, step = where(j)
        slot = j & (SLOTS - 1)
        at = slice(g * ROWS, (g + 1) * ROWS)
        query = q_wide[peer(step) * own + g // groups, pl.ds(phase * some + g % groups * ROWS, ROWS), :]
        query = jnp.concatenate([jnp.where(i, query, 0.0) for i in inside], 1).astype(jnp.bfloat16)
        key = keys[slot, g // groups, pl.ds(g % groups * span, span), :]
        scores = jnp.dot(query, key, preferred_element_type=jnp.float32) * head**-0.5
        high = jnp.max(scores, -1, keepdims=True)
        drawn = jnp.exp(scores - high)
        total = jnp.sum(drawn, -1, keepdims=True)
        weights[at, :] = drawn.astype(jnp.bfloat16)
        parts[phase * n + step, at, :] = jnp.where(lane == head, total, jnp.broadcast_to(high, lane.shape))

    def gather(j, g, drawn):
        values_g = values[j & (SLOTS - 1), g // groups, pl.ds(g % groups * span, span), :]
        sums = lax.dot_general(drawn, values_g, (((1,), (1,)), ((), ())), preferred_element_type=jnp.float32)
        mine = sums[:, :LANES]
        for block in range(1, span // LANES):
            mine = jnp.where(inside[block], sums[:, block * LANES : (block + 1) * LANES], mine)
        seen[g * ROWS : (g + 1) * ROWS, :] = mine

    def finish(j, mine):
        phase, step = where(j)
        for g in range(own * groups):
            at = slice(g * ROWS, (g + 1) * ROWS)
            turned = mine[at]
            for _ in range((LANES - head) // TURN):
                turned = pltpu.roll(turned, 0, 1, stride=TURN, stride_axis=0)
            parts[phase * n + step, at, :head] = turned[:, :head]

    def attend(j, behind, ahead):
        drawn = [weights[g * ROWS : (g + 1) * ROWS, :] for g in range(own * groups)]
        if behind:
            finish(j - 1, seen[...])
        for g in range(own * groups):
            if ahead:
                weigh(j + 1, g)
            gather(j, g, drawn[g])

    def send(phase, step):
        index = phase * n + step
        return pltpu.make_async_remote_copy(
            src_ref=parts.at[index],
            dst_ref=others.at[index],
            send_sem=send_sem.at[index],
            recv_sem=recv_sem.at[index],
            device_id={"sp": peer(step)},
            device_id_type=MESH,
        )

    def refill(j):
        @pl.when(j + 1 + SLOTS < units + PHASES)
        def _():
            fetch_k(j + 1 + SLOTS).start()

        @pl.when(j + SLOTS < units + PHASES)
        def _():
            fetch_v(j + SLOTS).start()

    def work(j, _):
        fetch_k(j + 1).wait()
        fetch_v(j).wait()
        attend(j, True, True)
        send(*where(j - 1)).start()
        refill(j)
        return 0

    def give(phase, step):
        index = phase * n + step
        return pltpu.make_async_remote_copy(
            src_ref=done.at[phase],
            dst_ref=out_ref.at[pl.ds(me * own, own), pl.ds(phase * some, some)],
            send_sem=out_send.at[index],
            recv_sem=out_recv.at[index],
            device_id={"sp": peer(step)},
            device_id_type=MESH,
        )

    def keep(phase):
        return pltpu.make_async_copy(done.at[phase], out_ref.at[pl.ds(me * own, own), pl.ds(phase * some, some)], own_sem.at[phase])

    def far(step):
        side = math.isqrt(n)
        return sum(min(d, side - d) for d in (step // side, step % side))

    def settle(phase):
        steps = [0] + [step for step in range(n - 1, 0, -1)]
        sums, top = None, None
        for some_steps in (steps[:-LATE], steps[-LATE:]):
            runs = []
            for step in some_steps:
                if step:
                    send(phase, step).wait_recv()
                runs.append((others if step else parts)[phase * n + step])
            highs = [jnp.broadcast_to(run[:, head + 1 : head + 2], run.shape) for run in runs]
            if sums is not None:
                runs.append(sums)
                highs.append(top)
            top = functools.reduce(jnp.maximum, highs)
            sums = sum(run * jnp.exp(high - top) for run, high in zip(runs, highs))
        result = sums[:, :head] / sums[:, head : head + 1]
        done[phase] = result.astype(jnp.bfloat16).reshape(own, some, head)
        for step in sorted(range(1, n), key=far, reverse=True):
            give(phase, step).start()
        keep(phase).start()

    fetch_k(0).wait()
    for g in range(own * groups):
        weigh(0, g)
    fetch_k(SLOTS).start()
    pl.semaphore_wait(barrier, n - 1)
    fetch_k(1).wait()
    fetch_v(0).wait()
    attend(0, False, True)
    refill(0)
    lax.fori_loop(1, units, work, 0)
    finish(units - 1, seen[...])
    send(*where(units - 1)).start()
    for phase in range(PHASES):
        j = units + phase
        ahead = phase + 1 < PHASES
        if ahead:
            fetch_k(j + 1).wait()
        fetch_v(j).wait()
        attend(j, False, ahead)
        finish(j, seen[...])
        settle(phase)

    def drain(index, _):
        phase, step = index // (n - 1), lax.rem(index, n - 1) + 1
        send(phase, step).wait_send()
        give(phase, step).wait()
        return 0

    lax.fori_loop(0, units, drain, 0)
    for phase in range(PHASES):
        keep(phase).wait()


def solution(mesh):
    n = mesh.shape["sp"]

    def step(q, k, v):
        batch, tokens, heads, head = k.shape
        own = batch // n
        some = heads // PHASES
        rows = own * some
        flat = lambda x: x.transpose(0, 2, 3, 1).reshape(batch, heads * head, tokens)
        return pl.pallas_call(
            functools.partial(kernel, n),
            out_shape=jax.ShapeDtypeStruct(q.shape, jnp.bfloat16),
            in_specs=[pl.BlockSpec(memory_space=pl.ANY)] * 3,
            out_specs=pl.BlockSpec(memory_space=pl.ANY),
            scratch_shapes=[
                pltpu.VMEM(q.shape, jnp.bfloat16),
                pltpu.VMEM((batch, heads, LANES), jnp.float32),
                pltpu.VMEM((SLOTS, own, some * head, tokens), jnp.bfloat16),
                pltpu.VMEM((SLOTS, own, some * head, tokens), jnp.bfloat16),
                pltpu.VMEM((rows, tokens), jnp.bfloat16),
                pltpu.VMEM((rows, LANES), jnp.float32),
                pltpu.VMEM((PHASES * n, rows, LANES), jnp.float32),
                pltpu.VMEM((PHASES * n, rows, LANES), jnp.float32),
                pltpu.VMEM((PHASES, own, some, head), jnp.bfloat16),
                pltpu.SemaphoreType.DMA,
                pltpu.SemaphoreType.DMA((SLOTS,)),
                pltpu.SemaphoreType.DMA((SLOTS,)),
                pltpu.SemaphoreType.DMA((PHASES * n,)),
                pltpu.SemaphoreType.DMA((PHASES * n,)),
                pltpu.SemaphoreType.DMA((PHASES * n,)),
                pltpu.SemaphoreType.DMA((PHASES * n,)),
                pltpu.SemaphoreType.DMA((PHASES,)),
            ],
            compiler_params=pltpu.CompilerParams(collective_id=0, has_side_effects=True, vmem_limit_bytes=48 * 2**20),
        )(q, flat(k), flat(v))

    return jax.shard_map(
        step,
        mesh=mesh,
        in_specs=(P("dp", None, None), P("dp", "sp", None, None), P("dp", "sp", None, None)),
        out_specs=P("dp", None, None),
        check_vma=False,
    )
```

```python
import functools
import math

import jax
import jax.numpy as jnp
from jax import lax
from jax.experimental import pallas as pl
from jax.experimental.pallas import tpu as pltpu
from jax.sharding import PartitionSpec as P

MESH = pl.DeviceIdType.MESH
LANES = 128
ROWS = 8
PHASES = 2
LATE = 3
SLOTS = 4


def kernel(
    n, q_hbm, k_hbm, v_hbm, out_ref, q_raw, q_wide, keys, values, weights, seen, parts, others, done, q_sem, k_sem, v_sem, send_sem, recv_sem, out_send, out_recv, own_sem
):
    batch, heads, head = q_hbm.shape
    own = batch // n
    some = heads // PHASES
    count = own * some
    groups = some // ROWS
    span = ROWS * head
    units = PHASES * (n - 1)
    me = lax.axis_index("sp")

    def peer(step):
        if n & (n - 1) == 0:
            return me ^ step
        return lax.rem(me + step, n)

    def where(j):
        if isinstance(j, int):
            return (j // (n - 1), n - 1 - j % (n - 1)) if j < units else (j - units, 0)
        phase = sum((j >= (n - 1) * p).astype(jnp.int32) for p in range(1, PHASES)) if PHASES > 1 else 0
        theirs = j < units
        return jnp.where(theirs, phase, j - units), jnp.where(theirs, n - 1 - j + phase * (n - 1), 0)

    def fetch(source, target, sem, j):
        phase, step = where(j)
        slot = j & (SLOTS - 1)
        rows = pl.ds(phase * (some * head), some * head)
        return pltpu.make_async_copy(source.at[pl.ds(peer(step) * own, own), rows], target.at[slot], sem.at[slot])

    fetch_k = functools.partial(fetch, k_hbm, keys, k_sem)
    fetch_v = functools.partial(fetch, v_hbm, values, v_sem)

    q_copy = pltpu.make_async_copy(q_hbm, q_raw, q_sem)
    q_copy.start()
    fetch_k(0).start()
    fetch_v(0).start()
    barrier = pltpu.get_barrier_semaphore()

    def greet(step, _):
        pl.semaphore_signal(barrier, inc=1, device_id={"sp": peer(step)}, device_id_type=MESH)
        return 0

    lax.fori_loop(1, n, greet, 0)
    for j in range(1, SLOTS):
        fetch_k(j).start()
        fetch_v(j).start()
    q_copy.wait()
    q_wide[:, :, :head] = q_raw[...].astype(jnp.float32)
    plain = q_wide[...].reshape(batch * heads, LANES)
    turned = plain
    turns = LANES // math.gcd(head, LANES)
    for h in range(1, turns):
        take = lax.rem(lax.broadcasted_iota(jnp.int32, plain.shape, 0), turns) == h
        turned = jnp.where(take, pltpu.roll(plain, h * head % LANES, 1), turned)
    q_wide[...] = turned.reshape(batch, heads, LANES)

    row = lax.broadcasted_iota(jnp.int32, (ROWS, LANES), 0)
    lane = lax.broadcasted_iota(jnp.int32, (ROWS, LANES), 1)
    inside = []
    for block in range(span // LANES):
        at = lane + block * LANES - row * head
        inside.append((at >= 0) & (at < head))

    def weigh(j, g):
        phase, step = where(j)
        slot = j & (SLOTS - 1)
        at = slice(g * ROWS, (g + 1) * ROWS)
        query = q_wide[peer(step) * own + g // groups, pl.ds(phase * some + g % groups * ROWS, ROWS), :]
        query = jnp.concatenate([jnp.where(i, query, 0.0) for i in inside], 1).astype(jnp.bfloat16)
        key = keys[slot, g // groups, pl.ds(g % groups * span, span), :]
        scores = jnp.dot(query, key, preferred_element_type=jnp.float32) * head**-0.5
        high = jnp.max(scores, -1, keepdims=True)
        drawn = jnp.exp(scores - high)
        total = jnp.sum(drawn, -1, keepdims=True)
        weights[at, :] = drawn.astype(jnp.bfloat16)
        parts[phase * n + step, at, :] = jnp.where(lane == head, total, jnp.broadcast_to(high, lane.shape))

    def gather(j, g, drawn):
        values_g = values[j & (SLOTS - 1), g // groups, pl.ds(g % groups * span, span), :]
        sums = lax.dot_general(drawn, values_g, (((1,), (1,)), ((), ())), preferred_element_type=jnp.float32)
        mine = sums[:, :LANES]
        for block in range(1, span // LANES):
            mine = jnp.where(inside[block], sums[:, block * LANES : (block + 1) * LANES], mine)
        seen[g * ROWS : (g + 1) * ROWS, :] = mine

    def finish(j, mine):
        phase, step = where(j)
        for g in range(own * groups):
            at = slice(g * ROWS, (g + 1) * ROWS)
            turned = mine[at]
            for h in range(1, turns):
                turned = jnp.where(row % turns == h, pltpu.roll(mine[at], -h * head % LANES, 1), turned)
            parts[phase * n + step, at, :head] = turned[:, :head]

    def attend(j, behind, ahead):
        drawn = [weights[g * ROWS : (g + 1) * ROWS, :] for g in range(own * groups)]
        if behind:
            finish(j - 1, seen[...])
        for g in range(own * groups):
            if ahead:
                weigh(j + 1, g)
            gather(j, g, drawn[g])

    def send(phase, step):
        index = phase * n + step
        return pltpu.make_async_remote_copy(
            src_ref=parts.at[index],
            dst_ref=others.at[index],
            send_sem=send_sem.at[index],
            recv_sem=recv_sem.at[index],
            device_id={"sp": peer(step)},
            device_id_type=MESH,
        )

    def refill(j):
        @pl.when(j + SLOTS < units + PHASES)
        def _():
            fetch_v(j + SLOTS).start()

        @pl.when(j + 1 + SLOTS < units + PHASES)
        def _():
            fetch_k(j + 1 + SLOTS).start()

    def work(j, _):
        fetch_k(j + 1).wait()
        fetch_v(j).wait()
        attend(j, True, True)
        send(*where(j - 1)).start()
        refill(j)
        return 0

    def give(phase, step):
        index = phase * n + step
        return pltpu.make_async_remote_copy(
            src_ref=done.at[phase],
            dst_ref=out_ref.at[pl.ds(me * own, own), pl.ds(phase * some, some)],
            send_sem=out_send.at[index],
            recv_sem=out_recv.at[index],
            device_id={"sp": peer(step)},
            device_id_type=MESH,
        )

    def keep(phase):
        return pltpu.make_async_copy(done.at[phase], out_ref.at[pl.ds(me * own, own), pl.ds(phase * some, some)], own_sem.at[phase])

    def far(step):
        side = math.isqrt(n)
        return sum(min(d, side - d) for d in (step // side, step % side))

    def arrive(phase, steps):
        for step in steps:
            send(phase, step).wait_recv()

    def merge(phase, steps, before):
        runs = [(others if step else parts)[phase * n + step] for step in steps]
        highs = [jnp.broadcast_to(run[:, head + 1 : head + 2], run.shape) for run in runs]
        totals = [jnp.broadcast_to(run[:, head : head + 1], run.shape) for run in runs]
        if before is not None:
            runs, highs, totals = runs + [before[0]], highs + [before[1]], totals + [before[2]]
        high = functools.reduce(jnp.maximum, highs)
        scales = [jnp.exp(h - high) for h in highs]
        return sum(r * x for r, x in zip(runs, scales)), high, sum(t * x for t, x in zip(totals, scales))

    def share(phase, merged):
        result = merged[0][:, :head] / merged[2][:, :head]
        done[phase] = result.astype(jnp.bfloat16).reshape(own, some, head)
        for step in reversed(by_distance):
            give(phase, step).start()
        keep(phase).start()

    fetch_k(0).wait()
    for g in range(own * groups):
        weigh(0, g)
    fetch_k(SLOTS).start()
    fetch_k(1).wait()
    fetch_v(0).wait()
    attend(0, False, True)
    refill(0)
    pl.semaphore_wait(barrier, n - 1)
    lax.fori_loop(1, units - 1, work, 0)

    by_distance = sorted(range(1, n), key=far)
    early = list(range(n - 1, LATE, -1))
    late = list(range(LATE, 0, -1))
    j = units - 1
    fetch_v(j).wait()
    attend(j, True, False)
    send(*where(j - 1)).start()
    finish(j, seen[...])
    send(*where(j)).start()
    fetch_k(units).wait()
    for g in range(own * groups):
        weigh(units, g)
    for phase in range(PHASES):
        j = units + phase
        ahead = phase + 1 < PHASES
        if ahead:
            fetch_k(j + 1).wait()
        if phase:
            arrive(phase - 1, early + late)
        fetch_v(j).wait()
        attend(j, False, ahead)
        if phase:
            share(phase - 1, merge(phase - 1, [0] + early + late, None))
        finish(j, seen[...])
    arrive(phase, early)
    merged = merge(phase, [0] + early, None)
    arrive(phase, late)
    share(phase, merge(phase, late, merged))

    for phase in range(PHASES):
        for step in range(1, n):
            send(phase, step).wait_send()
    for phase in range(PHASES):
        keep(phase).wait()
        for step in by_distance:
            give(phase, step).wait()


def solution(mesh):
    n = mesh.shape["sp"]

    def step(q, k, v):
        batch, tokens, heads, head = k.shape
        own = batch // n
        some = heads // PHASES
        rows = own * some
        flat = lambda x: x.transpose(0, 2, 3, 1).reshape(batch, heads * head, tokens)
        return pl.pallas_call(
            functools.partial(kernel, n),
            out_shape=jax.ShapeDtypeStruct(q.shape, jnp.bfloat16),
            in_specs=[pl.BlockSpec(memory_space=pl.ANY)] * 3,
            out_specs=pl.BlockSpec(memory_space=pl.ANY),
            scratch_shapes=[
                pltpu.VMEM(q.shape, jnp.bfloat16),
                pltpu.VMEM((batch, heads, LANES), jnp.float32),
                pltpu.VMEM((SLOTS, own, some * head, tokens), jnp.bfloat16),
                pltpu.VMEM((SLOTS, own, some * head, tokens), jnp.bfloat16),
                pltpu.VMEM((rows, tokens), jnp.bfloat16),
                pltpu.VMEM((rows, LANES), jnp.float32),
                pltpu.VMEM((PHASES * n, rows, LANES), jnp.float32),
                pltpu.VMEM((PHASES * n, rows, LANES), jnp.float32),
                pltpu.VMEM((PHASES, own, some, head), jnp.bfloat16),
                pltpu.SemaphoreType.DMA,
                pltpu.SemaphoreType.DMA((SLOTS,)),
                pltpu.SemaphoreType.DMA((SLOTS,)),
                pltpu.SemaphoreType.DMA((PHASES * n,)),
                pltpu.SemaphoreType.DMA((PHASES * n,)),
                pltpu.SemaphoreType.DMA((PHASES * n,)),
                pltpu.SemaphoreType.DMA((PHASES * n,)),
                pltpu.SemaphoreType.DMA((PHASES,)),
            ],
            compiler_params=pltpu.CompilerParams(collective_id=0, has_side_effects=True, vmem_limit_bytes=48 * 2**20),
        )(pltpu.with_memory_space_constraint(q, pltpu.HBM), flat(k), flat(v))

    return jax.shard_map(
        step,
        mesh=mesh,
        in_specs=(P("dp", None, None), P("dp", "sp", None, None), P("dp", "sp", None, None)),
        out_specs=P("dp", None, None),
        check_vma=False,
    )
```

```python
import functools
import math

import jax
import jax.numpy as jnp
from jax import lax
from jax.experimental import pallas as pl
from jax.experimental.pallas import tpu as pltpu
from jax.sharding import PartitionSpec as P

MESH = pl.DeviceIdType.MESH
LANES = 128
ROWS = 8
PHASES = 2
LATE = 3
SLOTS = 8


def kernel(
    n, q_hbm, k_hbm, v_hbm, out_ref, q_raw, q_wide, keys, values, weights, seen, parts, others, done, q_sem, k_sem, v_sem, send_sem, recv_sem, out_send, out_recv, own_sem
):
    batch, heads, head = q_hbm.shape
    own = batch // n
    some = heads // PHASES
    count = own * some
    groups = some // ROWS
    span = ROWS * head
    units = PHASES * (n - 1)
    me = lax.axis_index("sp")

    def peer(step):
        if n & (n - 1) == 0:
            return me ^ step
        return lax.rem(me + step, n)

    def where(j):
        if isinstance(j, int):
            return (j // (n - 1), n - 1 - j % (n - 1)) if j < units else (j - units, 0)
        phase = sum((j >= (n - 1) * p).astype(jnp.int32) for p in range(1, PHASES)) if PHASES > 1 else 0
        theirs = j < units
        return jnp.where(theirs, phase, j - units), jnp.where(theirs, n - 1 - j + phase * (n - 1), 0)

    def fetch(source, target, sem, j):
        phase, step = where(j)
        slot = j & (SLOTS - 1)
        rows = pl.ds(phase * (some * head), some * head)
        return pltpu.make_async_copy(source.at[pl.ds(peer(step) * own, own), rows], target.at[slot], sem.at[slot])

    fetch_k = functools.partial(fetch, k_hbm, keys, k_sem)
    fetch_v = functools.partial(fetch, v_hbm, values, v_sem)

    q_copy = pltpu.make_async_copy(q_hbm, q_raw, q_sem)
    q_copy.start()
    fetch_k(0).start()
    fetch_v(0).start()
    barrier = pltpu.get_barrier_semaphore()

    def greet(step, _):
        pl.semaphore_signal(barrier, inc=1, device_id={"sp": peer(step)}, device_id_type=MESH)
        return 0

    lax.fori_loop(1, n, greet, 0)
    for j in range(1, SLOTS):
        fetch_k(j).start()
        fetch_v(j).start()
    q_copy.wait()
    q_wide[:, :, :head] = q_raw[...].astype(jnp.float32)
    plain = q_wide[...].reshape(batch * heads, LANES)
    turned = plain
    turns = LANES // math.gcd(head, LANES)
    for h in range(1, turns):
        take = lax.rem(lax.broadcasted_iota(jnp.int32, plain.shape, 0), turns) == h
        turned = jnp.where(take, pltpu.roll(plain, h * head % LANES, 1), turned)
    q_wide[...] = turned.reshape(batch, heads, LANES)

    row = lax.broadcasted_iota(jnp.int32, (ROWS, LANES), 0)
    lane = lax.broadcasted_iota(jnp.int32, (ROWS, LANES), 1)
    inside = []
    for block in range(span // LANES):
        at = lane + block * LANES - row * head
        inside.append((at >= 0) & (at < head))

    def weigh(j, g):
        phase, step = where(j)
        slot = j & (SLOTS - 1)
        at = slice(g * ROWS, (g + 1) * ROWS)
        query = q_wide[peer(step) * own + g // groups, pl.ds(phase * some + g % groups * ROWS, ROWS), :]
        query = jnp.concatenate([jnp.where(i, query, 0.0) for i in inside], 1).astype(jnp.bfloat16)
        key = keys[slot, g // groups, pl.ds(g % groups * span, span), :]
        scores = jnp.dot(query, key, preferred_element_type=jnp.float32) * head**-0.5
        high = jnp.max(scores, -1, keepdims=True)
        drawn = jnp.exp(scores - high)
        total = jnp.sum(drawn, -1, keepdims=True)
        weights[at, :] = drawn.astype(jnp.bfloat16)
        parts[phase * n + step, at, :] = jnp.where(lane == head, total, jnp.broadcast_to(high, lane.shape))

    def gather(j, g, drawn):
        values_g = values[j & (SLOTS - 1), g // groups, pl.ds(g % groups * span, span), :]
        sums = lax.dot_general(drawn, values_g, (((1,), (1,)), ((), ())), preferred_element_type=jnp.float32)
        mine = sums[:, :LANES]
        for block in range(1, span // LANES):
            mine = jnp.where(inside[block], sums[:, block * LANES : (block + 1) * LANES], mine)
        seen[g * ROWS : (g + 1) * ROWS, :] = mine

    def finish(j, mine):
        phase, step = where(j)
        for g in range(own * groups):
            at = slice(g * ROWS, (g + 1) * ROWS)
            turned = mine[at]
            for h in range(1, turns):
                turned = jnp.where(row % turns == h, pltpu.roll(mine[at], -h * head % LANES, 1), turned)
            parts[phase * n + step, at, :head] = turned[:, :head]

    def attend(j, behind, ahead):
        drawn = [weights[g * ROWS : (g + 1) * ROWS, :] for g in range(own * groups)]
        if behind:
            finish(j - 1, seen[...])
        for g in range(own * groups):
            if ahead:
                weigh(j + 1, g)
            gather(j, g, drawn[g])

    def send(phase, step):
        index = phase * n + step
        return pltpu.make_async_remote_copy(
            src_ref=parts.at[index],
            dst_ref=others.at[index],
            send_sem=send_sem.at[index],
            recv_sem=recv_sem.at[index],
            device_id={"sp": peer(step)},
            device_id_type=MESH,
        )

    def refill(j):
        @pl.when(j + SLOTS < units + PHASES)
        def _():
            fetch_v(j + SLOTS).start()

        @pl.when(j + 1 + SLOTS < units + PHASES)
        def _():
            fetch_k(j + 1 + SLOTS).start()

    def work(j, _):
        fetch_k(j + 1).wait()
        fetch_v(j).wait()
        attend(j, True, True)
        send(*where(j - 1)).start()
        refill(j)
        return 0

    def give(phase, step):
        index = phase * n + step
        return pltpu.make_async_remote_copy(
            src_ref=done.at[phase],
            dst_ref=out_ref.at[pl.ds(me * own, own), pl.ds(phase * some, some)],
            send_sem=out_send.at[index],
            recv_sem=out_recv.at[index],
            device_id={"sp": peer(step)},
            device_id_type=MESH,
        )

    def keep(phase):
        return pltpu.make_async_copy(done.at[phase], out_ref.at[pl.ds(me * own, own), pl.ds(phase * some, some)], own_sem.at[phase])

    def far(step):
        side = math.isqrt(n)
        return sum(min(d, side - d) for d in (step // side, step % side))

    def arrive(phase, steps):
        for step in steps:
            send(phase, step).wait_recv()

    def merge(phase, steps, before):
        runs = [(others if step else parts)[phase * n + step] for step in steps]
        highs = [jnp.broadcast_to(run[:, head + 1 : head + 2], run.shape) for run in runs]
        totals = [jnp.broadcast_to(run[:, head : head + 1], run.shape) for run in runs]
        if before is not None:
            runs, highs, totals = runs + [before[0]], highs + [before[1]], totals + [before[2]]
        high = functools.reduce(jnp.maximum, highs)
        scales = [jnp.exp(h - high) for h in highs]
        return sum(r * x for r, x in zip(runs, scales)), high, sum(t * x for t, x in zip(totals, scales))

    def share(phase, merged):
        result = merged[0][:, :head] / merged[2][:, :head]
        done[phase] = result.astype(jnp.bfloat16).reshape(own, some, head)
        for step in reversed(by_distance):
            give(phase, step).start()
        keep(phase).start()

    fetch_k(0).wait()
    for g in range(own * groups):
        weigh(0, g)
    fetch_k(SLOTS).start()
    fetch_k(1).wait()
    fetch_v(0).wait()
    attend(0, False, True)
    refill(0)
    pl.semaphore_wait(barrier, n - 1)
    lax.fori_loop(1, units - 1, work, 0)

    by_distance = sorted(range(1, n), key=far)
    early = list(range(n - 1, LATE, -1))
    late = list(range(LATE, 0, -1))
    j = units - 1
    fetch_v(j).wait()
    attend(j, True, False)
    send(*where(j - 1)).start()
    finish(j, seen[...])
    send(*where(j)).start()
    fetch_k(units).wait()
    for g in range(own * groups):
        weigh(units, g)
    for phase in range(PHASES):
        j = units + phase
        ahead = phase + 1 < PHASES
        if ahead:
            fetch_k(j + 1).wait()
        if phase:
            arrive(phase - 1, early + late)
        fetch_v(j).wait()
        attend(j, False, ahead)
        if phase:
            share(phase - 1, merge(phase - 1, [0] + early + late, None))
        finish(j, seen[...])
    arrive(phase, early)
    merged = merge(phase, [0] + early, None)
    arrive(phase, late)
    share(phase, merge(phase, late, merged))

    for phase in range(PHASES):
        for step in range(1, n):
            send(phase, step).wait_send()
    for phase in range(PHASES):
        keep(phase).wait()
        for step in by_distance:
            give(phase, step).wait()


def solution(mesh):
    n = mesh.shape["sp"]

    def step(q, k, v):
        batch, tokens, heads, head = k.shape
        own = batch // n
        some = heads // PHASES
        rows = own * some
        flat = lambda x: x.transpose(0, 2, 3, 1).reshape(batch, heads * head, tokens)
        return pl.pallas_call(
            functools.partial(kernel, n),
            out_shape=jax.ShapeDtypeStruct(q.shape, jnp.bfloat16),
            in_specs=[pl.BlockSpec(memory_space=pl.ANY)] * 3,
            out_specs=pl.BlockSpec(memory_space=pl.ANY),
            scratch_shapes=[
                pltpu.VMEM(q.shape, jnp.bfloat16),
                pltpu.VMEM((batch, heads, LANES), jnp.float32),
                pltpu.VMEM((SLOTS, own, some * head, tokens), jnp.bfloat16),
                pltpu.VMEM((SLOTS, own, some * head, tokens), jnp.bfloat16),
                pltpu.VMEM((rows, tokens), jnp.bfloat16),
                pltpu.VMEM((rows, LANES), jnp.float32),
                pltpu.VMEM((PHASES * n, rows, LANES), jnp.float32),
                pltpu.VMEM((PHASES * n, rows, LANES), jnp.float32),
                pltpu.VMEM((PHASES, own, some, head), jnp.bfloat16),
                pltpu.SemaphoreType.DMA,
                pltpu.SemaphoreType.DMA((SLOTS,)),
                pltpu.SemaphoreType.DMA((SLOTS,)),
                pltpu.SemaphoreType.DMA((PHASES * n,)),
                pltpu.SemaphoreType.DMA((PHASES * n,)),
                pltpu.SemaphoreType.DMA((PHASES * n,)),
                pltpu.SemaphoreType.DMA((PHASES * n,)),
                pltpu.SemaphoreType.DMA((PHASES,)),
            ],
            compiler_params=pltpu.CompilerParams(collective_id=0, has_side_effects=True, vmem_limit_bytes=48 * 2**20),
        )(pltpu.with_memory_space_constraint(q, pltpu.HBM), flat(k), flat(v))

    return jax.shard_map(
        step,
        mesh=mesh,
        in_specs=(P("dp", None, None), P("dp", "sp", None, None), P("dp", "sp", None, None)),
        out_specs=P("dp", None, None),
        check_vma=False,
    )
```
